32 devices in a mesh: dp: 4 (over y, x), expert: 4 (over z), tensor: 2 (over core).
Axes of the slice: x: 2, y: 2, z: 4, core: 2. Of those that a mesh axis runs over, the one named last changes fastest.
Arguments:
- out_grad: bfloat16 [2048, 3584], P(('dp', 'expert'), 'tensor'), may hold values from -6 to 6
- routes: int32 [2048, 8], P(('dp', 'expert')), may hold values from 0 to 255, all different within a row; in each aligned block of 128 rows (0 to 127, 128 to 255, ...) at most 5 rows name the same one
- probs: float32 [2048, 8], P(('dp', 'expert')), may hold values from 0.1 to 1
- gate_pre: bfloat16 [4, 4, 20, 1024], P('dp', 'expert', None, 'tensor'), may hold values from -8 to 8
- up_pre: bfloat16 [4, 4, 20, 1024], P('dp', 'expert', None, 'tensor'), may hold values from -6 to 6
- gate_weight: bfloat16 [4, 3584, 1024], P('expert', None, 'tensor'), may hold values from -0.09375 to 0.09375
- up_weight: bfloat16 [4, 3584, 1024], P('expert', None, 'tensor'), may hold values from -0.09375 to 0.09375
- down_weight: bfloat16 [4, 1024, 3584], P('expert', 'tensor', 'dp'), may hold values from -0.1875 to 0.1875
Outputs:
- input_grad: bfloat16 [2048, 3584], P(('dp', 'expert'), 'tensor')
The draws below stay inside these ranges and needn't reach their ends.
Inputs may be any that keep to these rules, and one draw needn't show every extreme that they name: Each row names 8 different experts. In the 128 rows of one device no expert is named more than 5 times. Ids below 4 are the experts held here, expert e at index e of expert; routes to other ids leave no slot.
All inputs are finite; a program needn't handle non-finite values.
Results may differ from the reference program's by a relative error of at most 0.0072.
Values may be sent and summed in bfloat16 or wider, within the bound.
No kernel may reach another device: no remote copies, remote signals or barrier semaphores. Data moves between devices by JAX's collectives and lax.ppermute only.
A program may use at most 64 MiB of HBM per device.

```python
import math
import jax
import jax.numpy as jnp
import numpy as np
from jax import lax

D = 3584
FF = 1024
EXPERTS_ALL = 256
TOP = 8
TOK_DEV = 128
CAP = 5
EXPERTS = 4
SLOTS = 20
TOKENS = 2048
N_DP = 4
N_EXPERT = 4
N_TENSOR = 2


def levels(own_key, dims, shards, least, high):
    def one(dim, parts):
        draws = jax.random.uniform(jax.random.fold_in(jax.random.fold_in(own_key, 6), dim), (parts,), jnp.float32, least / len(shards), high / len(shards))
        return jnp.repeat(jnp.exp(draws), dims[dim] // parts).reshape((-1,) + (1,) * (len(dims) - dim - 1))

    factor_of = one(*shards[0])
    for cut in shards[1:]:
        factor_of = factor_of * one(*cut)
    return factor_of


def routed_block(stream_key, own, number, rows, count, top, most, lean):
    sequence = jax.random.permutation(stream_key, count)
    crowded, ordinary = shares(count, rows * top, most, lean, True), shares(count, rows * top, most, lean, False)
    places = jnp.arange(count)

    def named(lengths, offset_by):
        used = int((lengths > 0).sum())
        fixed = max(1, used // 4)
        shifted = fixed + (places - fixed + offset_by * (used - fixed)) % max(1, count - fixed)
        return jnp.zeros((count,), jnp.int32).at[sequence[jnp.where(places < fixed, places, shifted)]].set(jnp.asarray(lengths, jnp.int32))

    lengths = jnp.where(number % 4 == 0, named(crowded, number // 4), named(ordinary, number - number // 4 - 1))
    mixed = jax.random.permutation(jax.random.fold_in(own, 3), count)
    source_of, receiver = mixed[0:count // 2 * 2:2], mixed[1:count // 2 * 2:2]
    margin = jnp.minimum(lengths[source_of] - 1, most - lengths[receiver]) // 2
    margin = jnp.where((source_of == sequence[0]) | (receiver == sequence[0]) | (lengths[receiver] == 0), 0, jnp.maximum(margin, 0))
    shifted = jax.random.randint(jax.random.fold_in(own, 4), (count // 2,), 0, 1 << 20) % (margin + 1)
    lengths = lengths.at[source_of].add(-shifted).at[receiver].add(shifted)
    items = jnp.searchsorted(jnp.cumsum(lengths), jnp.arange(rows * top), side="right").astype(jnp.int32)
    table = items.reshape(top, rows).T
    table = table[jax.random.permutation(jax.random.fold_in(own, 1), rows)]
    offset_by = jax.random.randint(jax.random.fold_in(own, 2), (rows, 1), 0, top)
    return jnp.take_along_axis(table, (jnp.arange(top)[None, :] + offset_by) % top, axis=1)


def shares(number_of, total, reach, skew, full):
    portions = [(1 << 20) // math.isqrt(grade ** skew) + 1 for grade in range(1, number_of + 1)]
    largest = reach if full else min(reach, max(-(-total // number_of), total * portions[0] // sum(portions)))
    least = 1 if total - largest >= number_of - 1 else 0
    counts, rest = [largest] + [least] * (number_of - 1), total - largest - least * (number_of - 1)
    while rest > 0:
        candidates = [i for i in range(1, number_of) if counts[i] < largest] or [i for i in range(1, number_of) if counts[i] < reach]
        whole, remaining = sum([portions[i] for i in candidates]), rest
        for i in candidates:
            addition = min(reach - counts[i], max(1, remaining * portions[i] // whole), rest)
            counts[i] = counts[i] + addition
            rest = rest - addition
    return np.array(counts)


def centred(stream_key, shape, scale, limit, split=(), kind=jnp.bfloat16):
    values = scale * jax.random.normal(stream_key, shape, jnp.float32)
    if split:
        values = values * levels(stream_key, shape, split, -0.22, 0.18)
    return jnp.clip(values, -limit, limit).astype(kind)


def setup_inputs(seed: int = 0) -> dict:
    streams_of = jax.random.split(jax.random.key(seed), 9)
    out_grad = centred(streams_of[0], (TOKENS, D), 1.0, 6.0, ((0, 16), (1, 2)))
    routes_keys = jax.random.split(jax.random.fold_in(streams_of[1], 1), TOKENS // TOK_DEV)
    routes_turns = jax.random.permutation(jax.random.fold_in(streams_of[1], 3), TOKENS // TOK_DEV)
    routes = jax.vmap(lambda own, number: routed_block(jax.random.fold_in(streams_of[1], 2), own, number, TOK_DEV, EXPERTS_ALL, TOP, CAP, 2))(routes_keys, routes_turns).reshape((TOKENS, TOP))
    probs = jnp.clip(jnp.exp(math.log(1.0) - 2.3025851 * jax.random.uniform(streams_of[2], (TOKENS, TOP), jnp.float32) ** levels(streams_of[2], (TOKENS, TOP), ((0, 16),), -0.2, 0.2)), 0.1, 1.0)
    gate_pre = centred(streams_of[3], (N_DP, EXPERTS, SLOTS, FF), 2.0, 8.0, ((0, 4), (1, 4), (3, 2)))
    up_pre = centred(streams_of[4], (N_DP, EXPERTS, SLOTS, FF), 1.0, 6.0, ((0, 4), (1, 4), (3, 2)))
    gate_weight = centred(streams_of[5], (EXPERTS, D, FF), D ** -0.5, 0.09375, ((0, 4), (2, 2)))
    up_weight = centred(streams_of[6], (EXPERTS, D, FF), D ** -0.5, 0.09375, ((0, 4), (2, 2)))
    down_weight = centred(streams_of[7], (EXPERTS, FF, D), FF ** -0.5, 0.1875, ((0, 4), (1, 2), (2, 4)))
    return dict(out_grad=out_grad, routes=routes, probs=probs, gate_pre=gate_pre, up_pre=up_pre, gate_weight=gate_weight, up_weight=up_weight, down_weight=down_weight)


def slot_tables(block_routes, block_probs, experts, capacity):
    expert_ids = jnp.arange(experts, dtype=jnp.int32)
    matches = block_routes[:, :, None] == expert_ids[None, None, :]
    picked = jnp.sum(matches.astype(jnp.int32), axis=1)
    weight = jnp.sum(jnp.where(matches, block_probs[:, :, None], jnp.float32(0.0)), axis=1)
    before = jnp.cumsum(picked, axis=0) - picked
    rank_ids = jnp.arange(capacity, dtype=jnp.int32)
    select = (picked.T[:, None, :] == 1) & (before.T[:, None, :] == rank_ids[None, :, None])
    slot_scale = jnp.sum(jnp.where(select, weight.T[:, None, :], jnp.float32(0.0)), axis=2)
    return select, slot_scale


def expert_backward(slot_rows, gate_saved, up_saved, gate_matrix, up_matrix, down_matrix):
    hidden_grad = lax.dot_general(slot_rows, down_matrix, (((1,), (1,)), ((), ())), preferred_element_type=jnp.float32)
    gate_act = gate_saved.astype(jnp.float32)
    up_act = up_saved.astype(jnp.float32)
    sigmoid_gate = jax.nn.sigmoid(gate_act)
    activated = gate_act * sigmoid_gate
    derivative = sigmoid_gate * (1.0 + gate_act * (1.0 - sigmoid_gate))
    gate_grad = (hidden_grad * up_act * derivative).astype(jnp.bfloat16)
    up_grad = (hidden_grad * activated).astype(jnp.bfloat16)
    half_width = FF // N_TENSOR
    running = jnp.zeros((slot_rows.shape[0], D), jnp.float32)
    for piece_index in range(N_TENSOR):
        lower = piece_index * half_width
        upper = lower + half_width
        partial_value = lax.dot_general(gate_grad[:, lower:upper], gate_matrix[:, lower:upper], (((1,), (1,)), ((), ())), preferred_element_type=jnp.float32)
        partial_value = partial_value + lax.dot_general(up_grad[:, lower:upper], up_matrix[:, lower:upper], (((1,), (1,)), ((), ())), preferred_element_type=jnp.float32)
        rounded = lax.optimization_barrier(partial_value.astype(jnp.bfloat16))
        running = running + rounded.astype(jnp.float32)
    return running.astype(jnp.bfloat16)


def reference(out_grad, routes, probs, gate_pre, up_pre, gate_weight, up_weight, down_weight):
    group_grad = out_grad.reshape(N_DP, N_EXPERT, TOK_DEV, D)
    group_routes = routes.reshape(N_DP, N_EXPERT, TOK_DEV, TOP)
    group_probs = probs.reshape(N_DP, N_EXPERT, TOK_DEV, TOP)

    def group_backward(operands):
        grads_here, routes_here, probs_here, gate_here, up_here = operands
        select, slot_scale = jax.vmap(lambda rows_r, rows_p: slot_tables(rows_r, rows_p, N_EXPERT, CAP))(routes_here, probs_here)
        select_float = select.astype(jnp.float32)
        picked_rows = jnp.einsum('secT,sTd->secd', select_float, grads_here.astype(jnp.float32))
        outgoing = (slot_scale[..., None] * picked_rows).astype(jnp.bfloat16)
        arrived = jnp.transpose(outgoing, (1, 0, 2, 3)).reshape(N_EXPERT, N_EXPERT * CAP, D)
        returned_rows = lax.map(lambda inputs: expert_backward(*inputs), (arrived, gate_here, up_here, gate_weight, up_weight, down_weight))
        returned_rows = jnp.transpose(returned_rows.reshape(N_EXPERT, N_EXPERT, CAP, D), (1, 0, 2, 3))
        combined = jnp.einsum('secT,secd->sTd', select_float, returned_rows.astype(jnp.float32))
        return combined.astype(jnp.bfloat16)

    result = lax.map(group_backward, (group_grad, group_routes, group_probs, gate_pre, up_pre))
    return result.reshape(TOKENS, D)
```

```python
import jax
import jax.numpy as jnp
from jax import lax
from jax.sharding import PartitionSpec as P

CAP = 5
FEW = 8


def slot_tables(block_routes, block_probs, experts, capacity):
    expert_ids = jnp.arange(experts, dtype=jnp.int32)
    matches = block_routes[:, :, None] == expert_ids[None, None, :]
    picked = jnp.sum(matches.astype(jnp.int32), axis=1)
    weight = jnp.sum(jnp.where(matches, block_probs[:, :, None], jnp.float32(0.0)), axis=1)
    before = jnp.cumsum(picked, axis=0) - picked
    rank_ids = jnp.arange(capacity, dtype=jnp.int32)
    select = (picked.T[:, None, :] == 1) & (before.T[:, None, :] == rank_ids[None, :, None])
    slot_scale = jnp.sum(jnp.where(select, weight.T[:, None, :], jnp.float32(0.0)), axis=2)
    return (select, slot_scale)


def shifted(blocks, axis):
    count = lax.axis_size(axis)
    me = lax.axis_index(axis)
    own = lax.dynamic_index_in_dim(blocks, me, 0, keepdims=False)
    arrived = []
    for step in range(1, count):
        target = lax.rem(me + step, count)
        block = lax.dynamic_index_in_dim(blocks, target, 0, keepdims=False)
        arrived.append(lax.ppermute(block, axis, [(i, (i + step) % count) for i in range(count)]))
    return own, arrived


def local(out_grad, routes, probs, gate_pre, up_pre, gate_weight, up_weight, down_weight):
    experts = lax.axis_size("expert")
    groups = lax.axis_size("dp")
    select, slot_scale = slot_tables(routes, probs, experts, CAP)
    slot_count = experts * CAP
    slot_table = select.reshape(slot_count, -1).astype(jnp.bfloat16)
    picked_rows = jnp.dot(slot_table, out_grad, preferred_element_type=jnp.float32)
    outgoing = (slot_scale.reshape(-1, 1) * picked_rows).astype(jnp.bfloat16)
    rows = lax.all_gather(outgoing, "tensor", axis=1, tiled=True)
    width = rows.shape[1] // groups
    blocks = rows.reshape(experts, CAP, groups, width).transpose(2, 0, 1, 3)
    blocks = blocks.reshape(groups * experts, CAP, width)
    arrived = lax.all_to_all(blocks, ("dp", "expert"), split_axis=0, concat_axis=0, tiled=True)
    part = lax.dot_general(
        arrived.reshape(groups * slot_count, width),
        down_weight[0],
        (((1,), (1,)), ((), ())),
        preferred_element_type=jnp.float32,
    )
    part = part.astype(jnp.bfloat16).reshape(groups, slot_count, -1)
    if groups <= FEW:
        own, others = shifted(part, "dp")
        hidden_grad = own.astype(jnp.float32)
        for other in others:
            hidden_grad = hidden_grad + other.astype(jnp.float32)
    else:
        part = lax.all_to_all(part, "dp", split_axis=0, concat_axis=0, tiled=True)
        hidden_grad = jnp.sum(part.astype(jnp.float32), axis=0)
    gate_act = gate_pre[0, 0].astype(jnp.float32)
    up_act = up_pre[0, 0].astype(jnp.float32)
    sigmoid_gate = jax.nn.sigmoid(gate_act)
    activated = gate_act * sigmoid_gate
    derivative = sigmoid_gate * (1.0 + gate_act * (1.0 - sigmoid_gate))
    gate_grad = (hidden_grad * up_act * derivative).astype(jnp.bfloat16)
    up_grad = (hidden_grad * activated).astype(jnp.bfloat16)

    def back(weights):
        value = lax.dot_general(
            gate_grad, weights[0], (((1,), (1,)), ((), ())), preferred_element_type=jnp.float32
        )
        return value + lax.dot_general(
            up_grad, weights[1], (((1,), (1,)), ((), ())), preferred_element_type=jnp.float32
        )

    value = back((gate_weight[0], up_weight[0])).astype(jnp.bfloat16)
    halves = lax.axis_size("tensor")
    value = value.reshape(slot_count, halves, -1).transpose(1, 0, 2)
    own, others = shifted(value, "tensor")
    slot_grad = own.astype(jnp.float32)
    for other in others:
        slot_grad = slot_grad + other.astype(jnp.float32)
    slot_grad = slot_grad.astype(jnp.bfloat16).reshape(experts, CAP, -1)
    if experts <= FEW:
        own, others = shifted(slot_grad, "expert")
        me = lax.axis_index("expert")
        table = slot_table.reshape(experts, CAP, -1)
        tables = [
            lax.dynamic_index_in_dim(table, lax.rem(me + experts - i, experts), 0, keepdims=False)
            for i in range(experts)
        ]
        tables = jnp.concatenate(tables, axis=0)
        returned = jnp.concatenate([own] + others, axis=0)
    else:
        returned = lax.all_to_all(slot_grad, "expert", split_axis=0, concat_axis=0, tiled=True)
        returned = returned.reshape(slot_count, -1)
        tables = slot_table
    combined = lax.dot_general(
        tables, returned, (((0,), (0,)), ((), ())), preferred_element_type=jnp.float32
    )
    return combined.astype(jnp.bfloat16)


def solution(mesh):
    placed = (
        P(("dp", "expert"), "tensor"),
        P(("dp", "expert"), None),
        P(("dp", "expert"), None),
        P("dp", "expert", None, "tensor"),
        P("dp", "expert", None, "tensor"),
        P("expert", None, "tensor"),
        P("expert", None, "tensor"),
        P("expert", "tensor", "dp"),
    )
    return jax.shard_map(
        local, mesh=mesh, in_specs=placed, out_specs=P(("dp", "expert"), "tensor"), check_vma=False
    )
```

```python
import functools

import jax
import jax.numpy as jnp
from jax import lax
from jax.experimental import pallas as pl
from jax.experimental.pallas import tpu as pltpu
from jax.sharding import PartitionSpec as P


CAP = 5
ROWS = 8
FEW = 8
MIB = 1 << 20


def slot_tables(block_routes, block_probs, experts, capacity):
    expert_ids = jnp.arange(experts, dtype=jnp.int32)
    matches = block_routes[:, :, None] == expert_ids[None, None, :]
    picked = jnp.sum(matches.astype(jnp.int32), axis=1)
    weight = jnp.sum(jnp.where(matches, block_probs[:, :, None], jnp.float32(0.0)), axis=1)
    before = jnp.cumsum(picked, axis=0) - picked
    rank_ids = jnp.arange(capacity, dtype=jnp.int32)
    select = (picked.T[:, None, :] == 1) & (before.T[:, None, :] == rank_ids[None, :, None])
    slot_scale = jnp.sum(jnp.where(select, weight.T[:, None, :], jnp.float32(0.0)), axis=2)
    return (select, slot_scale)


def shifted(blocks, axis):
    count = lax.axis_size(axis)
    me = lax.axis_index(axis)
    own = lax.dynamic_index_in_dim(blocks, me, 0, keepdims=False)
    arrived = []
    for step in range(1, count):
        target = lax.rem(me + step, count)
        block = lax.dynamic_index_in_dim(blocks, target, 0, keepdims=False)
        arrived.append(lax.ppermute(block, axis, [(i, (i + step) % count) for i in range(count)]))
    return own, arrived


def exchanged_whole(out_grad, routes, probs, gate_pre, up_pre, gate_weight, up_weight, down_weight):
    experts = lax.axis_size("expert")
    groups = lax.axis_size("dp")
    select, slot_scale = slot_tables(routes, probs, experts, CAP)
    slot_count = experts * CAP
    slot_table = select.reshape(slot_count, -1).astype(jnp.bfloat16)
    picked_rows = jnp.dot(slot_table, out_grad, preferred_element_type=jnp.float32)
    outgoing = (slot_scale.reshape(-1, 1) * picked_rows).astype(jnp.bfloat16)
    rows = lax.all_gather(outgoing, "tensor", axis=1, tiled=True)
    width = rows.shape[1] // groups
    blocks = rows.reshape(experts, CAP, groups, width).transpose(2, 0, 1, 3)
    blocks = blocks.reshape(groups * experts, CAP, width)
    arrived = lax.all_to_all(blocks, ("dp", "expert"), split_axis=0, concat_axis=0, tiled=True)
    part = lax.dot_general(
        arrived.reshape(groups * slot_count, width),
        down_weight[0],
        (((1,), (1,)), ((), ())),
        preferred_element_type=jnp.float32,
    )
    part = part.astype(jnp.bfloat16).reshape(groups, slot_count, -1)
    if groups <= FEW:
        own, others = shifted(part, "dp")
        hidden_grad = own.astype(jnp.float32)
        for other in others:
            hidden_grad = hidden_grad + other.astype(jnp.float32)
    else:
        part = lax.all_to_all(part, "dp", split_axis=0, concat_axis=0, tiled=True)
        hidden_grad = jnp.sum(part.astype(jnp.float32), axis=0)
    gate_act = gate_pre[0, 0].astype(jnp.float32)
    up_act = up_pre[0, 0].astype(jnp.float32)
    sigmoid_gate = jax.nn.sigmoid(gate_act)
    activated = gate_act * sigmoid_gate
    derivative = sigmoid_gate * (1.0 + gate_act * (1.0 - sigmoid_gate))
    gate_grad = (hidden_grad * up_act * derivative).astype(jnp.bfloat16)
    up_grad = (hidden_grad * activated).astype(jnp.bfloat16)

    def back(weights):
        value = lax.dot_general(
            gate_grad, weights[0], (((1,), (1,)), ((), ())), preferred_element_type=jnp.float32
        )
        return value + lax.dot_general(
            up_grad, weights[1], (((1,), (1,)), ((), ())), preferred_element_type=jnp.float32
        )

    value = back((gate_weight[0], up_weight[0])).astype(jnp.bfloat16)
    halves = lax.axis_size("tensor")
    value = value.reshape(slot_count, halves, -1).transpose(1, 0, 2)
    own, others = shifted(value, "tensor")
    slot_grad = own.astype(jnp.float32)
    for other in others:
        slot_grad = slot_grad + other.astype(jnp.float32)
    slot_grad = slot_grad.astype(jnp.bfloat16).reshape(experts, CAP, -1)
    if experts <= FEW:
        own, others = shifted(slot_grad, "expert")
        me = lax.axis_index("expert")
        table = slot_table.reshape(experts, CAP, -1)
        tables = [
            lax.dynamic_index_in_dim(table, lax.rem(me + experts - i, experts), 0, keepdims=False)
            for i in range(experts)
        ]
        tables = jnp.concatenate(tables, axis=0)
        returned = jnp.concatenate([own] + others, axis=0)
    else:
        returned = lax.all_to_all(slot_grad, "expert", split_axis=0, concat_axis=0, tiled=True)
        returned = returned.reshape(slot_count, -1)
        tables = slot_table
    combined = lax.dot_general(
        tables, returned, (((0,), (0,)), ((), ())), preferred_element_type=jnp.float32
    )
    return combined.astype(jnp.bfloat16)


HELD = pl.BlockSpec(memory_space=pltpu.VMEM)
FAR = pl.BlockSpec(memory_space=pltpu.HBM)
LOOSE = pl.BlockSpec(memory_space=pl.ANY)


def call(kernel, outs, specs, mib, scratch=()):
    return pl.pallas_call(
        kernel,
        out_shape=outs,
        in_specs=specs,
        out_specs=[HELD] * len(outs),
        scratch_shapes=list(scratch),
        compiler_params=pltpu.CompilerParams(vmem_limit_bytes=mib * MIB),
    )


def far(value):
    return pltpu.with_memory_space_constraint(value, pltpu.HBM)


def transposed(a, b):
    return lax.dot_general(a, b, (((1,), (1,)), ((), ())), preferred_element_type=jnp.float32)


def ahead(place, step, count):
    if count & (count - 1):
        return (place + step) % count if isinstance(place, int) else lax.rem(place + step, count)
    return place ^ step


def behind(place, step, count):
    return ahead(place, (count - step) if count & (count - 1) else step, count)


def dispatch_kernel(experts, routes_far, probs_far, grad_far, table_ref, *refs):
    block_refs, (routes_ref, probs_ref, grad_ref, arrived) = refs[:experts], refs[experts:]
    copies = [
        pltpu.make_async_copy(source, near, arrived.at[k])
        for k, (source, near) in enumerate(
            [(routes_far, routes_ref), (probs_far, probs_ref), (grad_far, grad_ref)]
        )
    ]
    for copy in copies:
        copy.start()
    me = lax.axis_index("expert")
    tokens = grad_ref.shape[0]
    earlier = lax.broadcasted_iota(jnp.int32, (tokens, tokens), 0) < lax.broadcasted_iota(
        jnp.int32, (tokens, tokens), 1
    )
    earlier = jnp.where(earlier, 1.0, 0.0).astype(jnp.bfloat16)
    rank = lax.broadcasted_iota(jnp.int32, (ROWS, tokens), 0)
    rank = jnp.where(rank < CAP, rank.astype(jnp.float32), -1.0)
    copies[0].wait()
    copies[1].wait()
    routes = routes_ref[...]
    probs = probs_ref[...]
    matches = [routes == ahead(me, i, experts) for i in range(experts)]
    picked = jnp.concatenate(
        [jnp.max(jnp.where(m, 1.0, 0.0), axis=0, keepdims=True) for m in matches], axis=0
    )
    before = jnp.dot(picked.astype(jnp.bfloat16), earlier, preferred_element_type=jnp.float32)
    tables, scales = [], []
    for i in range(experts):
        weight = jnp.sum(jnp.where(matches[i], probs, 0.0), axis=0, keepdims=True)
        chosen = (before[i : i + 1] == rank) & (picked[i : i + 1] > 0.5)
        tables.append(jnp.where(chosen, 1.0, 0.0))
        scales.append(jnp.sum(jnp.where(chosen, weight, 0.0), axis=1, keepdims=True))
    table = jnp.concatenate(tables, axis=0).astype(jnp.bfloat16)
    table_ref[...] = table
    copies[2].wait()
    rows = jnp.dot(table, grad_ref[...], preferred_element_type=jnp.float32)
    rows = rows * jnp.concatenate(scales, axis=0)
    for i in range(experts):
        block_refs[i][...] = rows[i * ROWS : (i + 1) * ROWS].astype(jnp.bfloat16)


def stack_kernel(*refs):
    blocks, out_ref = refs[1:-1], refs[-1]
    for j, block in enumerate(blocks):
        out_ref[j * ROWS : (j + 1) * ROWS, :] = block[...]


def column_kernel(halves, inner, *refs):
    stacks, pieces = refs[:halves], refs[halves:]
    width = pieces[0].shape[1]
    core = lax.axis_index("tensor")
    high_place, low_place = (f(lax.axis_index("dp"), inner) for f in (lax.div, lax.rem))
    for high in range(halves):
        half = ahead(high_place, high, halves)
        for turn in range(halves):

            @pl.when(half == behind(core, turn, halves))
            def _():
                for low in range(inner):
                    first = pl.multiple_of(ahead(low_place, low, inner) * width, width)
                    pieces[high * inner + low][...] = stacks[turn][:, pl.ds(first, width)]


def factor_kernel(
    experts, gate_far, up_far, down_far, after, gate_factor_ref, up_factor_ref, down_ref,
    gate_ref, up_ref, arrived,
):
    copies = [
        pltpu.make_async_copy(source, near, arrived.at[k])
        for k, (source, near) in enumerate(
            [(gate_far, gate_ref), (up_far, up_ref), (down_far, down_ref)]
        )
    ]
    for copy in copies:
        copy.start()
    me = lax.axis_index("expert")
    row = lax.broadcasted_iota(jnp.int32, (experts * ROWS, experts * CAP), 0)
    slot = lax.broadcasted_iota(jnp.int32, (experts * ROWS, experts * CAP), 1)
    rank = lax.rem(row, ROWS)
    source = behind(me, lax.div(row, ROWS), experts)
    taken = (slot == source * CAP + rank) & (rank < CAP)
    place = jnp.where(taken, 1.0, 0.0).astype(jnp.bfloat16)
    copies[0].wait()
    copies[1].wait()
    gate = jnp.dot(place, gate_ref[...], preferred_element_type=jnp.float32)
    up = jnp.dot(place, up_ref[...], preferred_element_type=jnp.float32)
    sigmoid = jax.nn.sigmoid(gate)
    gate_factor_ref[...] = up * (sigmoid * (1.0 + gate * (1.0 - sigmoid)))
    up_factor_ref[...] = gate * sigmoid
    copies[2].wait()


def fetch_kernel(far, after, near, arrived):
    copy = pltpu.make_async_copy(far, near, arrived)
    copy.start()
    copy.wait()


def hidden_kernel(*refs):
    count = len(refs) // 2 - 1
    arrived, down_ref, outs = refs[:count], refs[count], refs[count + 2 :]
    rows = arrived[0].shape[0]
    together = jnp.concatenate([a[...] for a in arrived], axis=0)
    part = transposed(together, down_ref[...])
    for k, out in enumerate(outs):
        out[...] = part[k * rows : (k + 1) * rows].astype(out.dtype)


def feature_kernel(offset, halves, *refs):
    parts, (gate_factor, up_factor, gate_weight, up_weight, out_ref) = refs[:-5], refs[-5:]
    hidden = parts[0][...].astype(jnp.float32)
    for part in parts[1:]:
        hidden = hidden + part[...].astype(jnp.float32)
    gate_grad = (hidden * gate_factor[...]).astype(jnp.bfloat16)
    up_grad = (hidden * up_factor[...]).astype(jnp.bfloat16)
    width = out_ref.shape[1]
    first = ahead(lax.axis_index("tensor"), offset, halves) * width
    span = pl.ds(pl.multiple_of(first, width), width)
    value = transposed(gate_grad, gate_weight[span, :]) + transposed(up_grad, up_weight[span, :])
    out_ref[...] = value.astype(jnp.bfloat16)


def moved(value, axis, step, back=False):
    count = lax.axis_size(axis)
    to = behind if back else ahead
    return lax.ppermute(value, axis, [(i, to(i, step, count)) for i in range(count)])


def exchanged(out_grad, routes, probs, gate_pre, up_pre, gate_weight, up_weight, down_weight):
    experts, groups, halves = (lax.axis_size(a) for a in ("expert", "dp", "tensor"))
    tokens, half = out_grad.shape
    inner = groups // halves
    hidden, width = down_weight.shape[1:]
    if experts > FEW or groups > FEW or groups % halves or half != inner * width or width % 128:
        return exchanged_whole(
            out_grad, routes, probs, gate_pre, up_pre, gate_weight, up_weight, down_weight
        )
    rows = experts * ROWS
    bf16 = functools.partial(jax.ShapeDtypeStruct, dtype=jnp.bfloat16)
    f32 = functools.partial(jax.ShapeDtypeStruct, dtype=jnp.float32)
    copies = pltpu.SemaphoreType.DMA

    table, *blocks = call(
        functools.partial(dispatch_kernel, experts),
        [bf16((rows, tokens))] + [bf16((ROWS, half))] * experts,
        [FAR] * 3,
        8,
        [
            pltpu.VMEM(routes.T.shape, routes.dtype),
            pltpu.VMEM(probs.T.shape, probs.dtype),
            pltpu.VMEM(out_grad.shape, out_grad.dtype),
            copies((3,)),
        ],
    )(far(routes.T), far(probs.T), far(out_grad))
    own = blocks[0]
    blocks = [own] + [moved(blocks[i], "expert", i) for i in range(1, experts)]
    slots = gate_pre.shape[2:]
    gate_factor, up_factor, down = call(
        functools.partial(factor_kernel, experts),
        [f32((rows, hidden))] * 2 + [bf16((hidden, width))],
        [FAR] * 3 + [LOOSE],
        8,
        [pltpu.VMEM(slots, gate_pre.dtype), pltpu.VMEM(slots, up_pre.dtype), copies((3,))],
    )(far(gate_pre[0, 0]), far(up_pre[0, 0]), far(down_weight[0]), own)
    stack = call(stack_kernel, [bf16((rows, half))], [LOOSE] + [HELD] * experts, 8)(
        gate_factor, *blocks
    )[0]
    stacks = [stack] + [moved(stack, "tensor", turn) for turn in range(1, halves)]
    pieces = call(
        functools.partial(column_kernel, halves, inner),
        [bf16((rows, width))] * groups,
        [HELD] * halves,
        8,
    )(*stacks)
    fetch = call(fetch_kernel, [bf16(gate_weight.shape[1:])], [FAR, LOOSE], 8, [copies])
    gate_held = fetch(far(gate_weight[0]), pieces[0])[0]

    def spread(values, to):
        out = [values[0]]
        for high in range(halves):
            for low in range(inner):
                if high or low:
                    pairs = []
                    for g in range(groups):
                        d = to(g // inner, high, halves) * inner + to(g % inner, low, inner)
                        pairs.append((g, d))
                    k = high * inner + low
                    out.append(lax.ppermute(values[k], "dp", pairs))
        return out

    parts = call(
        hidden_kernel,
        [f32((rows, hidden))] + [bf16((rows, hidden))] * (groups - 1),
        [HELD] * (groups + 1) + [LOOSE],
        8,
    )(*spread(pieces, ahead), down, gate_held)
    sums = spread(parts, behind)
    up_held = fetch(far(up_weight[0]), parts[-1])[0]
    shares = []
    for offset in range(halves - 1, -1, -1):
        value = call(
            functools.partial(feature_kernel, offset, halves),
            [bf16((rows, half))],
            [HELD] * (groups + 4),
            16,
        )(*sums, gate_factor, up_factor, gate_held, up_held)[0]
        shares.append(moved(value, "tensor", offset) if offset else value)
    slot_grad = sum(share.astype(jnp.float32) for share in shares).astype(jnp.bfloat16)
    returned = [slot_grad[j * ROWS : (j + 1) * ROWS] for j in range(experts)]
    returned = [returned[0]] + [
        moved(returned[j], "expert", j, back=True) for j in range(1, experts)
    ]
    combined = lax.dot_general(
        table,
        jnp.concatenate(returned, axis=0),
        (((0,), (0,)), ((), ())),
        preferred_element_type=jnp.float32,
    )
    return combined.astype(jnp.bfloat16)


def solution(mesh):
    placed = (
        P(("dp", "expert"), "tensor"),
        P(("dp", "expert"), None),
        P(("dp", "expert"), None),
        P("dp", "expert", None, "tensor"),
        P("dp", "expert", None, "tensor"),
        P("expert", None, "tensor"),
        P("expert", None, "tensor"),
        P("expert", "tensor", "dp"),
    )
    return jax.shard_map(
        exchanged, mesh=mesh, in_specs=placed, out_specs=P(("dp", "expert"), "tensor"), check_vma=False
    )
```

```python
import functools

import jax
import jax.numpy as jnp
from jax import lax
from jax.experimental import pallas as pl
from jax.experimental.pallas import tpu as pltpu
from jax.sharding import PartitionSpec as P


CAP = 5
ROWS = 8
FEW = 8
MIB = 1 << 20


def slot_tables(block_routes, block_probs, experts, capacity):
    expert_ids = jnp.arange(experts, dtype=jnp.int32)
    matches = block_routes[:, :, None] == expert_ids[None, None, :]
    picked = jnp.sum(matches.astype(jnp.int32), axis=1)
    weight = jnp.sum(jnp.where(matches, block_probs[:, :, None], jnp.float32(0.0)), axis=1)
    before = jnp.cumsum(picked, axis=0) - picked
    rank_ids = jnp.arange(capacity, dtype=jnp.int32)
    select = (picked.T[:, None, :] == 1) & (before.T[:, None, :] == rank_ids[None, :, None])
    slot_scale = jnp.sum(jnp.where(select, weight.T[:, None, :], jnp.float32(0.0)), axis=2)
    return (select, slot_scale)


def shifted(blocks, axis):
    count = lax.axis_size(axis)
    me = lax.axis_index(axis)
    own = lax.dynamic_index_in_dim(blocks, me, 0, keepdims=False)
    arrived = []
    for step in range(1, count):
        target = lax.rem(me + step, count)
        block = lax.dynamic_index_in_dim(blocks, target, 0, keepdims=False)
        arrived.append(lax.ppermute(block, axis, [(i, (i + step) % count) for i in range(count)]))
    return own, arrived


def exchanged_whole(out_grad, routes, probs, gate_pre, up_pre, gate_weight, up_weight, down_weight):
    experts = lax.axis_size("expert")
    groups = lax.axis_size("dp")
    select, slot_scale = slot_tables(routes, probs, experts, CAP)
    slot_count = experts * CAP
    slot_table = select.reshape(slot_count, -1).astype(jnp.bfloat16)
    picked_rows = jnp.dot(slot_table, out_grad, preferred_element_type=jnp.float32)
    outgoing = (slot_scale.reshape(-1, 1) * picked_rows).astype(jnp.bfloat16)
    rows = lax.all_gather(outgoing, "tensor", axis=1, tiled=True)
    width = rows.shape[1] // groups
    blocks = rows.reshape(experts, CAP, groups, width).transpose(2, 0, 1, 3)
    blocks = blocks.reshape(groups * experts, CAP, width)
    arrived = lax.all_to_all(blocks, ("dp", "expert"), split_axis=0, concat_axis=0, tiled=True)
    part = lax.dot_general(
        arrived.reshape(groups * slot_count, width),
        down_weight[0],
        (((1,), (1,)), ((), ())),
        preferred_element_type=jnp.float32,
    )
    part = part.astype(jnp.bfloat16).reshape(groups, slot_count, -1)
    if groups <= FEW:
        own, others = shifted(part, "dp")
        hidden_grad = own.astype(jnp.float32)
        for other in others:
            hidden_grad = hidden_grad + other.astype(jnp.float32)
    else:
        part = lax.all_to_all(part, "dp", split_axis=0, concat_axis=0, tiled=True)
        hidden_grad = jnp.sum(part.astype(jnp.float32), axis=0)
    gate_act = gate_pre[0, 0].astype(jnp.float32)
    up_act = up_pre[0, 0].astype(jnp.float32)
    sigmoid_gate = jax.nn.sigmoid(gate_act)
    activated = gate_act * sigmoid_gate
    derivative = sigmoid_gate * (1.0 + gate_act * (1.0 - sigmoid_gate))
    gate_grad = (hidden_grad * up_act * derivative).astype(jnp.bfloat16)
    up_grad = (hidden_grad * activated).astype(jnp.bfloat16)

    def back(weights):
        value = lax.dot_general(
            gate_grad, weights[0], (((1,), (1,)), ((), ())), preferred_element_type=jnp.float32
        )
        return value + lax.dot_general(
            up_grad, weights[1], (((1,), (1,)), ((), ())), preferred_element_type=jnp.float32
        )

    value = back((gate_weight[0], up_weight[0])).astype(jnp.bfloat16)
    halves = lax.axis_size("tensor")
    value = value.reshape(slot_count, halves, -1).transpose(1, 0, 2)
    own, others = shifted(value, "tensor")
    slot_grad = own.astype(jnp.float32)
    for other in others:
        slot_grad = slot_grad + other.astype(jnp.float32)
    slot_grad = slot_grad.astype(jnp.bfloat16).reshape(experts, CAP, -1)
    if experts <= FEW:
        own, others = shifted(slot_grad, "expert")
        me = lax.axis_index("expert")
        table = slot_table.reshape(experts, CAP, -1)
        tables = [
            lax.dynamic_index_in_dim(table, lax.rem(me + experts - i, experts), 0, keepdims=False)
            for i in range(experts)
        ]
        tables = jnp.concatenate(tables, axis=0)
        returned = jnp.concatenate([own] + others, axis=0)
    else:
        returned = lax.all_to_all(slot_grad, "expert", split_axis=0, concat_axis=0, tiled=True)
        returned = returned.reshape(slot_count, -1)
        tables = slot_table
    combined = lax.dot_general(
        tables, returned, (((0,), (0,)), ((), ())), preferred_element_type=jnp.float32
    )
    return combined.astype(jnp.bfloat16)


HELD = pl.BlockSpec(memory_space=pltpu.VMEM)
FAR = pl.BlockSpec(memory_space=pltpu.HBM)
LOOSE = pl.BlockSpec(memory_space=pl.ANY)


def call(kernel, outs, specs, mib, scratch=()):
    return pl.pallas_call(
        kernel,
        out_shape=outs,
        in_specs=specs,
        out_specs=[HELD] * len(outs),
        scratch_shapes=list(scratch),
        compiler_params=pltpu.CompilerParams(vmem_limit_bytes=mib * MIB),
    )


def far(value):
    return pltpu.with_memory_space_constraint(value, pltpu.HBM)


def transposed(a, b):
    return lax.dot_general(a, b, (((1,), (1,)), ((), ())), preferred_element_type=jnp.float32)


def dispatch_kernel(experts, routes_far, probs_far, grad_far, table_ref, *refs):
    block_refs, (routes_ref, probs_ref, grad_ref, arrived) = refs[:experts], refs[experts:]
    copies = [
        pltpu.make_async_copy(source, near, arrived.at[k])
        for k, (source, near) in enumerate(
            [(routes_far, routes_ref), (probs_far, probs_ref), (grad_far, grad_ref)]
        )
    ]
    for copy in copies:
        copy.start()
    me = lax.axis_index("expert")
    tokens = grad_ref.shape[0]
    earlier = lax.broadcasted_iota(jnp.int32, (tokens, tokens), 0) < lax.broadcasted_iota(
        jnp.int32, (tokens, tokens), 1
    )
    earlier = jnp.where(earlier, 1.0, 0.0).astype(jnp.bfloat16)
    rank = lax.broadcasted_iota(jnp.int32, (ROWS, tokens), 0)
    rank = jnp.where(rank < CAP, rank.astype(jnp.float32), -1.0)
    copies[0].wait()
    copies[1].wait()
    routes = routes_ref[...]
    probs = probs_ref[...]
    matches = [routes == (me ^ i) for i in range(experts)]
    picked = jnp.concatenate(
        [jnp.max(jnp.where(m, 1.0, 0.0), axis=0, keepdims=True) for m in matches], axis=0
    )
    before = jnp.dot(picked.astype(jnp.bfloat16), earlier, preferred_element_type=jnp.float32)
    tables, scales = [], []
    for i in range(experts):
        weight = jnp.sum(jnp.where(matches[i], probs, 0.0), axis=0, keepdims=True)
        chosen = (before[i : i + 1] == rank) & (picked[i : i + 1] > 0.5)
        tables.append(jnp.where(chosen, 1.0, 0.0))
        scales.append(jnp.sum(jnp.where(chosen, weight, 0.0), axis=1, keepdims=True))
    table = jnp.concatenate(tables, axis=0).astype(jnp.bfloat16)
    table_ref[...] = table
    copies[2].wait()
    rows = jnp.dot(table, grad_ref[...], preferred_element_type=jnp.float32)
    rows = rows * jnp.concatenate(scales, axis=0)
    for i in range(experts):
        block_refs[i][...] = rows[i * ROWS : (i + 1) * ROWS].astype(jnp.bfloat16)


def stack_kernel(*refs):
    blocks, out_ref = refs[1:-1], refs[-1]
    for j, block in enumerate(blocks):
        out_ref[j * ROWS : (j + 1) * ROWS, :] = block[...]


def column_kernel(inner, own, other, *pieces):
    width = pieces[0].shape[1]
    core, place = lax.axis_index("tensor"), lax.axis_index("dp")
    rest = slice(ROWS, own.shape[0])
    for k, piece in enumerate(pieces):
        holder = place ^ k
        first = pl.multiple_of(lax.rem(holder, inner) * width, width)
        span = pl.ds(first, width)

        @pl.when(lax.div(holder, inner) == core)
        def _():
            piece[:ROWS, :] = own[:ROWS, span]
            piece[rest, :] = other[rest, span]

        @pl.when(lax.div(holder, inner) != core)
        def _():
            piece[:ROWS, :] = other[:ROWS, span]
            piece[rest, :] = own[rest, span]


def factor_kernel(
    experts, gate_far, up_far, down_far, after, gate_factor_ref, up_factor_ref, down_ref,
    gate_ref, up_ref, arrived,
):
    copies = [
        pltpu.make_async_copy(source, near, arrived.at[k])
        for k, (source, near) in enumerate(
            [(gate_far, gate_ref), (up_far, up_ref), (down_far, down_ref)]
        )
    ]
    for copy in copies:
        copy.start()
    me = lax.axis_index("expert")
    row = lax.broadcasted_iota(jnp.int32, (experts * ROWS, experts * CAP), 0)
    slot = lax.broadcasted_iota(jnp.int32, (experts * ROWS, experts * CAP), 1)
    rank = lax.rem(row, ROWS)
    source = me ^ lax.div(row, ROWS)
    taken = (slot == source * CAP + rank) & (rank < CAP)
    place = jnp.where(taken, 1.0, 0.0).astype(jnp.bfloat16)
    copies[0].wait()
    copies[1].wait()
    gate = jnp.dot(place, gate_ref[...], preferred_element_type=jnp.float32)
    up = jnp.dot(place, up_ref[...], preferred_element_type=jnp.float32)
    sigmoid = jax.nn.sigmoid(gate)
    gate_factor_ref[...] = up * (sigmoid * (1.0 + gate * (1.0 - sigmoid)))
    up_factor_ref[...] = gate * sigmoid
    copies[2].wait()


def fetch_kernel(far, after, near, arrived):
    copy = pltpu.make_async_copy(far, near, arrived)
    copy.start()
    copy.wait()


def hidden_kernel(*refs):
    count = (len(refs) - 3) // 2
    arrived, (down, other_down), outs = refs[:count], refs[count : count + 2], refs[count + 3 :]
    rows = arrived[0].shape[0]
    together = jnp.concatenate([a[...] for a in arrived[1:]], axis=0)
    part = transposed(together, other_down[...])
    for k, out in enumerate(outs[1:]):
        out[...] = part[k * rows : (k + 1) * rows].astype(out.dtype)
    outs[0][...] = transposed(arrived[0][...], down[...])


def feature_kernel(offset, *refs):
    parts, (gate_factor, up_factor, gate_weight, up_weight, out_ref) = refs[:-5], refs[-5:]
    hidden = parts[0][...].astype(jnp.float32)
    for part in parts[1:]:
        hidden = hidden + part[...].astype(jnp.float32)
    gate_grad = (hidden * gate_factor[...]).astype(jnp.bfloat16)
    up_grad = (hidden * up_factor[...]).astype(jnp.bfloat16)
    width = out_ref.shape[1]
    first = (lax.axis_index("tensor") ^ offset) * width
    span = pl.ds(pl.multiple_of(first, width), width)
    value = transposed(gate_grad, gate_weight[span, :]) + transposed(up_grad, up_weight[span, :])
    out_ref[...] = value.astype(jnp.bfloat16)


def swapped(value):
    return lax.ppermute(value, "tensor", [(0, 1), (1, 0)])


def crossed(values, axis):
    out = [values[0]]
    for k in range(1, len(values)):
        pairs = [(i * 2 + t, (i ^ k) * 2 + 1 - t) for i in range(len(values)) for t in range(2)]
        out.append(lax.ppermute(values[k], (axis, "tensor"), pairs))
    return out


def suits(experts, groups, halves):
    return all(n <= FEW and n & (n - 1) == 0 for n in (experts, groups)) and halves == 2 <= groups


def exchanged(out_grad, routes, probs, gate_pre, up_pre, gate_weight, up_weight, down_weight):
    experts, groups, halves = (lax.axis_size(a) for a in ("expert", "dp", "tensor"))
    tokens, half = out_grad.shape
    inner = groups // halves
    hidden, width = down_weight.shape[1:]
    if not suits(experts, groups, halves) or half != inner * width or width % 128:
        return exchanged_whole(
            out_grad, routes, probs, gate_pre, up_pre, gate_weight, up_weight, down_weight
        )
    rows = experts * ROWS
    bf16 = functools.partial(jax.ShapeDtypeStruct, dtype=jnp.bfloat16)
    f32 = functools.partial(jax.ShapeDtypeStruct, dtype=jnp.float32)
    copies = pltpu.SemaphoreType.DMA

    table, *blocks = call(
        functools.partial(dispatch_kernel, experts),
        [bf16((rows, tokens))] + [bf16((ROWS, half))] * experts,
        [FAR] * 3,
        8,
        [
            pltpu.VMEM(routes.T.shape, routes.dtype),
            pltpu.VMEM(probs.T.shape, probs.dtype),
            pltpu.VMEM(out_grad.shape, out_grad.dtype),
            copies((3,)),
        ],
    )(far(routes.T), far(probs.T), far(out_grad))
    own = blocks[0]
    blocks = crossed(blocks, "expert")
    other_down = swapped(down_weight[0])
    slots = gate_pre.shape[2:]
    gate_factor, up_factor, down = call(
        functools.partial(factor_kernel, experts),
        [f32((rows, hidden))] * 2 + [bf16((hidden, width))],
        [FAR] * 3 + [LOOSE],
        8,
        [pltpu.VMEM(slots, gate_pre.dtype), pltpu.VMEM(slots, up_pre.dtype), copies((3,))],
    )(far(gate_pre[0, 0]), far(up_pre[0, 0]), far(down_weight[0]), own)
    stack = call(stack_kernel, [bf16((rows, half))], [LOOSE] + [HELD] * experts, 8)(
        gate_factor, *blocks
    )[0]
    pieces = call(
        functools.partial(column_kernel, inner), [bf16((rows, width))] * groups, [HELD] * 2, 8
    )(stack, swapped(stack))
    fetch = call(fetch_kernel, [bf16(gate_weight.shape[1:])], [FAR, LOOSE], 8, [copies])
    gate_held = fetch(far(gate_weight[0]), pieces[0])[0]

    parts = call(
        hidden_kernel,
        [f32((rows, hidden))] + [bf16((rows, hidden))] * (groups - 1),
        [HELD] * (groups + 2) + [LOOSE],
        8,
    )(*crossed(pieces, "dp"), down, other_down, gate_held)
    sums = crossed(parts, "dp")
    up_held = fetch(far(up_weight[0]), parts[-1])[0]
    shares = []
    for offset in range(halves):
        value = call(
            functools.partial(feature_kernel, offset),
            [bf16((rows, half))],
            [HELD] * (groups + 4),
            16,
        )(*sums, gate_factor, up_factor, gate_held, up_held)[0]
        shares.append(value if offset else swapped(value))
    slot_grad = sum(share.astype(jnp.float32) for share in shares).astype(jnp.bfloat16)
    returned = [slot_grad[j * ROWS : (j + 1) * ROWS] for j in range(experts)]
    returned = crossed(returned, "expert")
    returned[0] = swapped(returned[0])
    combined = lax.dot_general(
        table,
        jnp.concatenate(returned, axis=0),
        (((0,), (0,)), ((), ())),
        preferred_element_type=jnp.float32,
    )
    return combined.astype(jnp.bfloat16)


def solution(mesh):
    placed = (
        P(("dp", "expert"), "tensor"),
        P(("dp", "expert"), None),
        P(("dp", "expert"), None),
        P("dp", "expert", None, "tensor"),
        P("dp", "expert", None, "tensor"),
        P("expert", None, "tensor"),
        P("expert", None, "tensor"),
        P("expert", "tensor", "dp"),
    )
    step = jax.shard_map(
        exchanged, mesh=mesh, in_specs=placed, out_specs=P(("dp", "expert"), "tensor"), check_vma=False
    )
    experts, groups = mesh.shape["expert"], mesh.shape["dp"]
    if not suits(experts, groups, mesh.shape["tensor"]):
        return step
    return step
```
